512 devices in a mesh: grp: 2 (over y), ka: 32 (over z), orb: 4 (over x), band: 2 (over core).
Axes of the slice: x: 4, y: 2, z: 32, core: 2. Of those that a mesh axis runs over, the one named last changes fastest.
The devices are a block of a 4x8x32 slice.
Arguments:
- eigvecs: bfloat16 [64, 2, 8192, 256], P(('grp', 'ka'), None, 'orb', 'band'), parts along dimension 0, may hold values from -0.03515625 to 0.03515625
- band_rank: int32 [64, 256], P(('grp', 'ka'), 'band'), parts along dimension 0, may hold values from 0 to 255, each once within a row
- occ_count: int32 [2], P('grp'), parts along dimension 0, may hold values from 128 to 256
- wrap_shift: int32 [2], P('grp'), parts along dimension 0, may hold values from 1 to 4095
- orbital_site: int32 [16384], P(('grp', 'orb')), parts along dimension 0, may hold values from 0 to 63
Outputs:
- wilson: float32 [64, 256, 2, 256], P(('grp', 'ka'), 'orb', None, 'band'), parts along dimension 0
The draws below stay inside these ranges and needn't reach their ends.
There are 2 independent parts, one for each index of `grp`. The reference program is written for one: setup_inputs(seed, part) draws one part's arguments, and reference() takes and returns one part's arrays. A program takes and returns all parts, laid end to end along the dimension named above; each array names one. Nothing has to cross between parts.
All inputs are finite; a program needn't handle non-finite values.
Results may differ from the reference program's by a relative error of at most 0.025.
Values may be sent and summed in bfloat16 or wider, within the bound.
No kernel may reach another device: no remote copies, remote signals or barrier semaphores. Data moves between devices by JAX's collectives and lax.ppermute only.
A program may use at most 64 MiB of HBM per device.

```python
import math
import jax
import jax.numpy as jnp
from jax import lax

ORBS = 8192
BANDS = 256
NS_STEPS = 8
SITES = 64
KPTS = 32


def draw_eigvecs(key, part):
    entry_scale = (2.0 * ORBS) ** (-0.5)
    full_shape = (KPTS, 2, ORBS, BANDS)
    base_key = jax.random.fold_in(key, 101)
    noise_key = jax.random.fold_in(key, 202)
    mix_key = jax.random.fold_in(key, 303)
    common = jax.random.normal(base_key, (2, ORBS, BANDS), jnp.float32)
    fresh_noise = jax.random.normal(noise_key, full_shape, jnp.float32)
    mixing = jax.random.uniform(mix_key, (KPTS, 1, 1, 1), jnp.float32, 0.3, 0.55)
    values = mixing * common[None] + jnp.sqrt(1.0 - mixing * mixing) * fresh_noise
    return (jnp.clip(values, -4.4, 4.4) * entry_scale).astype(jnp.bfloat16)


def set_ends(array, key, smallest, largest):
    spot = [jax.random.randint(jax.random.fold_in(key, axis), (), 0, length) for axis, length in enumerate(array.shape)]
    main_axis = array.shape.index(max(array.shape))
    next_to = spot[:main_axis] + [(spot[main_axis] + 1) % array.shape[main_axis]] + spot[main_axis + 1:]
    return array.at[tuple(spot)].set(smallest).at[tuple(next_to)].set(largest)


def setup_inputs(seed: int = 0, part: int = 0) -> dict:
    streams_of = jax.random.split(jax.random.key(seed), 6)
    part_splits = jax.random.split(jax.random.fold_in(streams_of[5], part), 6)
    eigvecs = draw_eigvecs(jax.random.fold_in(jax.random.fold_in(streams_of[5], part), 71), part)
    band_rank = jax.vmap(lambda own: jax.random.permutation(own, BANDS))(jax.random.split(part_splits[1], KPTS)).reshape((KPTS, BANDS)).astype(jnp.int32)
    occ_count = jax.random.randint(part_splits[2], (1,), BANDS // 2, BANDS + 1).astype(jnp.int32)
    wrap_shift = jax.random.randint(part_splits[3], (1,), 1, 4096).astype(jnp.int32)
    orbital_site = set_ends(jax.random.randint(part_splits[4], (ORBS,), 0, SITES), jax.random.fold_in(part_splits[4], 1), 0, SITES - 1).astype(jnp.int32)
    return dict(eigvecs=eigvecs, band_rank=band_rank, occ_count=occ_count, wrap_shift=wrap_shift, orbital_site=orbital_site)


ns_gain = 0.7
eps_mean = 1e-06

def complex_block(matrix):
    order_size = matrix.shape[0]
    real_part = matrix[:, :order_size]
    imag_part = matrix[:, order_size:]
    upper_half = jnp.concatenate([real_part, imag_part], axis=1)
    lower_half = jnp.concatenate([-imag_part, real_part], axis=1)
    return jnp.concatenate([upper_half, lower_half], axis=0)

def complex_product(left_side, right_side):
    return jnp.dot(left_side, complex_block(right_side), precision=lax.Precision.HIGHEST, preferred_element_type=jnp.float32)

def polar_step(iterate):
    order_size = iterate.shape[1]
    rounded = iterate.astype(jnp.bfloat16)
    widened = rounded.astype(jnp.float32)
    gram_matrix = jnp.einsum('kri,krj->kij', widened, widened, precision=lax.Precision.HIGHEST)
    gram_real = gram_matrix[:, :order_size, :order_size] + gram_matrix[:, order_size:, order_size:]
    gram_imag = gram_matrix[:, :order_size, order_size:] - gram_matrix[:, order_size:, :order_size]
    upper_half = jnp.concatenate([gram_real, gram_imag], axis=2)
    lower_half = jnp.concatenate([-gram_imag, gram_real], axis=2)
    gram_block = jnp.concatenate([upper_half, lower_half], axis=1).astype(jnp.bfloat16).astype(jnp.float32)
    product = jnp.einsum('kri,kij->krj', widened, gram_block, precision=lax.Precision.HIGHEST)
    return 1.5 * iterate - 0.5 * product

def margin_pair(block_pair):
    left_block, right_block = block_pair
    stacked = jnp.concatenate([left_block[0], left_block[1]], axis=0)
    real_side = jnp.concatenate([right_block[0], right_block[1]], axis=0)
    imag_side = jnp.concatenate([right_block[1], -right_block[0]], axis=0)
    paired = jnp.concatenate([real_side, imag_side], axis=1)
    return jnp.dot(stacked.T, paired, preferred_element_type=jnp.float32)

def reference(eigvecs, band_rank, occ_count, wrap_shift, orbital_site):
    occupied = band_rank < occ_count[0]
    masked = jnp.where(occupied[:, None, None, :], eigvecs, jnp.zeros((), jnp.bfloat16))
    phase_angle = (wrap_shift[0] * orbital_site % SITES).astype(jnp.float32) * (2.0 * math.pi / SITES)
    cosine = jnp.cos(phase_angle)[:, None]
    sine_factor = jnp.sin(phase_angle)[:, None]
    first_real = masked[0, 0].astype(jnp.float32)
    first_imag = masked[0, 1].astype(jnp.float32)
    wrapped = jnp.stack([cosine * first_real + sine_factor * first_imag, cosine * first_imag - sine_factor * first_real]).astype(jnp.bfloat16)
    right_blocks = jnp.concatenate([masked[1:], wrapped[None]], axis=0)
    margins = lax.map(margin_pair, (masked, right_blocks))
    occupied_total = occ_count[0].astype(jnp.float32)
    squares = lax.optimization_barrier(jnp.sum(margins * margins, axis=(1, 2)))
    iterate = margins * (ns_gain * lax.rsqrt(squares / occupied_total + eps_mean))[:, None, None]
    for sweep_index in range(NS_STEPS):
        iterate = polar_step(iterate)
    identity = jnp.concatenate([jnp.eye(BANDS, dtype=jnp.float32), jnp.zeros((BANDS, BANDS), jnp.float32)], axis=1)

    def link(running, factor):
        following = complex_product(running, factor)
        return (following, following)
    final_loop, prefix = lax.scan(link, identity, iterate)
    return prefix.reshape(KPTS, BANDS, 2, BANDS) * math.sqrt(BANDS)
```

```python
import functools
import math

import jax
import jax.numpy as jnp
from jax import lax
from jax.experimental import pallas as pl
from jax.experimental.pallas import tpu as pltpu
from jax.sharding import PartitionSpec as P

NS_STEPS = 8
SITES = 64


ns_gain = 0.7
eps_mean = 1e-06


def shifted(value, axis, by):
    count = lax.axis_size(axis)
    return lax.ppermute(value, axis, [(i, (i + by) % count) for i in range(count)])


def carried(value, axis, by):
    count = lax.axis_size(axis)
    return lax.ppermute(value, axis, [(i, i + by) for i in range(count - by)])


def from_everyone(value, axis):
    count = lax.axis_size(axis)
    return lax.all_to_all(
        jnp.broadcast_to(value[None], (count, *value.shape)), axis, 0, 0, tiled=True
    )


def polar_kernel(occ_ref, margin_ref, out_ref):
    half = margin_ref.shape[2]
    real = jnp.concatenate([margin_ref[0, 0], margin_ref[1, 0]], axis=1)
    imag = jnp.concatenate([margin_ref[0, 1], margin_ref[1, 1]], axis=1)
    squares = jnp.sum(real * real + imag * imag)
    scale = ns_gain * lax.rsqrt(
        jnp.full((1, 1), squares, jnp.float32) / occ_ref[0].astype(jnp.float32) + eps_mean
    )
    iterate = jnp.concatenate([real, imag], axis=0) * scale

    def step(index, iterate):
        real = iterate[:half].astype(jnp.bfloat16)
        imag = iterate[half:].astype(jnp.bfloat16)
        wide = jnp.concatenate([real, imag], axis=1)
        turned = jnp.concatenate([imag, -real], axis=1)
        gram = lax.dot_general(
            jnp.concatenate([wide, turned], axis=0),
            wide,
            (((1,), (1,)), ((), ())),
            preferred_element_type=jnp.float32,
        ).astype(jnp.bfloat16)
        gram_real, gram_imag = (gram[:half], gram[half:])
        block = jnp.concatenate(
            [
                jnp.concatenate([gram_real, -gram_imag], axis=1),
                jnp.concatenate([gram_imag, gram_real], axis=1),
            ],
            axis=0,
        )
        product = jnp.dot(
            block, jnp.concatenate([real, imag], axis=0), preferred_element_type=jnp.float32
        )
        return 1.5 * iterate - 0.5 * product

    iterate = lax.fori_loop(0, NS_STEPS, step, iterate)
    out_ref[...] = jnp.concatenate([iterate[:half], iterate[half:]], axis=1).astype(out_ref.dtype)


def polar_factor(margins, occ_count):
    order_size = margins.shape[2]
    return pl.pallas_call(
        polar_kernel,
        out_shape=jax.ShapeDtypeStruct((order_size, 2 * order_size), jnp.bfloat16),
        in_specs=[
            pl.BlockSpec(memory_space=pltpu.SMEM),
            pl.BlockSpec(memory_space=pltpu.VMEM),
        ],
        out_specs=pl.BlockSpec(memory_space=pltpu.VMEM),
        name="polar",
    )(occ_count, margins)


def product_kernel(joins_ref, left_ref, right_ref, own_ref, out_ref):
    rows, double = left_ref.shape
    order_size = double // 2
    stacked = jnp.concatenate([left_ref[:, :order_size], left_ref[:, order_size:]], axis=0)
    product = jnp.dot(stacked, right_ref[...], preferred_element_type=jnp.float32)
    real = product[:rows, :order_size] - product[rows:, order_size:]
    imag = product[:rows, order_size:] + product[rows:, :order_size]
    following = jnp.concatenate([real, imag], axis=1)
    own = own_ref[...].astype(jnp.float32)
    out_ref[...] = jnp.where(joins_ref[0] > 0, following, own).astype(out_ref.dtype)


def joined(left, right, own, joins, dtype):
    return pl.pallas_call(
        product_kernel,
        out_shape=jax.ShapeDtypeStruct(left.shape, dtype),
        in_specs=[pl.BlockSpec(memory_space=pltpu.SMEM)]
        + [pl.BlockSpec(memory_space=pltpu.VMEM)] * 3,
        out_specs=pl.BlockSpec(memory_space=pltpu.VMEM),
        name="joined",
    )(joins.astype(jnp.int32).reshape(1), left, right, own)


def margin_left(block, band_rank, wrap_shift, orbital_site):
    at_end = lax.axis_index("ka") == lax.axis_size("ka") - 1
    phase_angle = (wrap_shift[0] * orbital_site % SITES).astype(jnp.float32) * (
        2.0 * math.pi / SITES
    )
    cosine = jnp.cos(phase_angle)[:, None]
    sine_factor = jnp.sin(phase_angle)[:, None]
    real = block[0].astype(jnp.float32)
    imag = block[1].astype(jnp.float32)
    turned = jnp.stack([cosine * real - sine_factor * imag, cosine * imag + sine_factor * real])
    own = jnp.where(at_end, turned.astype(jnp.bfloat16), block)
    other = shifted(own, "band", 1)
    first = lax.axis_index("band") == 0
    low, high = (jnp.where(first, own, other), jnp.where(first, other, own))
    real_side = jnp.concatenate([low, high], axis=2)
    orbital_rows = block.shape[1]
    real_side = real_side.reshape(2 * orbital_rows, real_side.shape[2])
    imag_side = jnp.concatenate([-real_side[orbital_rows:], real_side[:orbital_rows]], axis=0)
    return lax.optimization_barrier(jnp.concatenate([real_side, imag_side], axis=1))


def body(eigvecs, band_rank, occ_count, wrap_shift, orbital_site):
    band_cols = eigvecs.shape[3]
    band_total = band_cols * lax.axis_size("band")
    block = eigvecs[0]
    place = lax.axis_index("ka")
    points = lax.axis_size("ka")
    arrived = shifted(block, "ka", -1)
    occupied = (band_rank < occ_count[0]).astype(jnp.float32)
    occupied_next = shifted(occupied, "ka", -1)
    occupied_rows = lax.all_gather(occupied[0], "band", tiled=True)
    lefts = margin_left(block, band_rank, wrap_shift, orbital_site)
    partial = lax.dot_general(
        lefts,
        arrived.reshape(lefts.shape[0], band_cols),
        (((0,), (0,)), ((), ())),
        preferred_element_type=jnp.float32,
    )
    partials = from_everyone(partial.astype(jnp.bfloat16), "orb")
    summed = partials.astype(jnp.float32).sum(axis=0).reshape(2, band_total, band_cols)
    summed = summed * (occupied_rows[:, None] * occupied_next)[None]
    margins = lax.all_gather(summed, "band")
    whole = polar_factor(margins, occ_count)
    shares = lax.axis_size("orb") * lax.axis_size("band")
    share = band_total // shares
    mine = lax.axis_index("orb") * lax.axis_size("band") + lax.axis_index("band")
    reach = 1
    half = band_total // lax.axis_size("band")
    sent = lax.dynamic_slice_in_dim(whole, lax.axis_index("band") * half, half, 0)
    before = lax.all_gather(carried(sent, "ka", reach), "band", tiled=True)
    whole = joined(before, whole, whole, place >= reach, jnp.bfloat16)
    rows = lax.dynamic_slice_in_dim(whole, mine * share, share, 0)
    reach *= 2
    while reach < points:
        before = carried(rows, "ka", reach)
        if reach > 2:
            whole = from_everyone(rows, ("orb", "band")).reshape(whole.shape)
        last = 2 * reach >= points
        rows = joined(
            before, whole, rows, place >= reach, jnp.float32 if last else jnp.bfloat16
        )
        reach *= 2
    loops = lax.all_gather(rows, "band", tiled=True).reshape(-1, 2, band_total)
    result = lax.dynamic_slice_in_dim(loops, lax.axis_index("band") * band_cols, band_cols, 2)
    return result[None] * math.sqrt(band_total)


def solution(mesh):
    return jax.shard_map(
        body,
        mesh=mesh,
        in_specs=(
            P(("grp", "ka"), None, "orb", "band"),
            P(("grp", "ka"), "band"),
            P("grp"),
            P("grp"),
            P(("grp", "orb")),
        ),
        out_specs=P(("grp", "ka"), "orb", None, "band"),
        check_vma=False,
    )
```
